64 devices in a mesh: batch: 4 (over x, y), graph: 16 (over z, core).
Axes of the slice: x: 2, y: 2, z: 8, core: 2. Of those that a mesh axis runs over, the one named last changes fastest.
The devices are a block of a 4x4x8 slice.
Arguments:
- features: bfloat16 [131072, 500], P(('batch', 'graph')), parts along dimension 0
- w_msg1: bfloat16 [500, 256], replicated
- w_self1: bfloat16 [500, 256], replicated
- w_msg2: bfloat16 [256, 256], replicated
- w_self2: bfloat16 [256, 256], replicated
- src_local: int32 [64, 20480], P(('batch', 'graph')), parts along dimension 0
- send_slot: int32 [64, 20480], P(('batch', 'graph')), parts along dimension 0
- edge_weight: float32 [64, 20480], P(('batch', 'graph')), parts along dimension 0
- recv_row: int32 [64, 16, 512], P(('batch', 'graph')), parts along dimension 0
Outputs:
- output: bfloat16 [131072, 256], P(('batch', 'graph')), parts along dimension 0
There are 4 independent parts. The reference program is written for one: setup_inputs(seed, part) draws one part's arguments, and reference() takes and returns one part's arrays. A program takes and returns all parts, laid end to end along the dimension named above; an argument that names none is the same for every part.
All inputs are finite; a program needn't handle non-finite values.
Results may differ from the reference program's by a relative error of at most 0.00844026.
Values are sent between devices in bfloat16 or wider.
A program may use at most 768 MiB of HBM per device.

```python
import jax
import jax.numpy as jnp
from jax import lax

GRAPH_DEVS = 16
NODES_DEV = 2048
DEGREE = 10
SLOT_CAP = 512
D_IN = 500
D_HID = 256
EDGES_DEV = NODES_DEV * DEGREE
HUB_SLOTS = SLOT_CAP // 8


def draw_graph(graph_key):
    sub_keys = jax.random.split(graph_key, 8)
    perm_keys = jax.random.split(sub_keys[0], GRAPH_DEVS)
    row_perm = jax.vmap(lambda one_key: jax.random.permutation(one_key, jnp.arange(NODES_DEV, dtype=jnp.int32)))(perm_keys)
    shifts = jax.random.randint(sub_keys[1], (GRAPH_DEVS, GRAPH_DEVS), 0, 4, dtype=jnp.int32)
    shifts = shifts * (1 - jnp.eye(GRAPH_DEVS, dtype=jnp.int32))
    counts = SLOT_CAP // jnp.left_shift(jnp.ones_like(shifts), shifts)
    offsets = jax.random.randint(sub_keys[2], (GRAPH_DEVS, GRAPH_DEVS, 1), 0, NODES_DEV - HUB_SLOTS, dtype=jnp.int32)
    slot_pos = jnp.arange(SLOT_CAP, dtype=jnp.int32)[None, None, :]
    tail_pos = HUB_SLOTS + (offsets + slot_pos - HUB_SLOTS) % (NODES_DEV - HUB_SLOTS)
    positions = jnp.where(slot_pos < HUB_SLOTS, slot_pos, tail_pos)
    dest_rows = jax.vmap(lambda perm_row, pos_row: perm_row[pos_row])(row_perm, positions)
    live_slot = slot_pos < jnp.transpose(counts)[:, :, None]
    recv_row = jnp.where(live_slot, dest_rows, NODES_DEV).astype(jnp.int32)
    sender = jnp.arange(GRAPH_DEVS, dtype=jnp.int32)[:, None]
    owner_draw = jax.random.randint(sub_keys[3], (GRAPH_DEVS, EDGES_DEV), 0, 2 * GRAPH_DEVS, dtype=jnp.int32)
    owner = jnp.where(owner_draw < GRAPH_DEVS, owner_draw, sender)
    limit = jnp.take_along_axis(counts, owner, axis=1)
    first = jax.random.randint(sub_keys[4], (GRAPH_DEVS, EDGES_DEV), 0, limit, dtype=jnp.int32)
    second = jax.random.randint(sub_keys[5], (GRAPH_DEVS, EDGES_DEV), 0, limit, dtype=jnp.int32)
    within = jnp.minimum(first, second)
    send_slot = (owner * SLOT_CAP + within).astype(jnp.int32)
    src_local = jax.random.randint(sub_keys[6], (GRAPH_DEVS, EDGES_DEV), 0, NODES_DEV, dtype=jnp.int32)
    dst_global = owner * NODES_DEV + recv_row[owner, sender, within]
    in_degree = jax.ops.segment_sum(jnp.ones((GRAPH_DEVS * EDGES_DEV,), jnp.int32), dst_global.reshape(-1), num_segments=GRAPH_DEVS * NODES_DEV)
    scale = jax.random.uniform(sub_keys[7], (GRAPH_DEVS, EDGES_DEV), jnp.float32, 0.5, 1.5)
    edge_weight = scale * lax.rsqrt(in_degree[dst_global].astype(jnp.float32))
    return src_local, send_slot, edge_weight, recv_row


def setup_inputs(seed: int = 0, part: int = 0) -> dict:
    base_key = jax.random.key(seed)
    weight_keys = jax.random.split(base_key, 4)
    part_keys = jax.random.split(jax.random.fold_in(base_key, part), 2)
    features = jax.random.normal(part_keys[0], (GRAPH_DEVS * NODES_DEV, D_IN), jnp.float32).astype(jnp.bfloat16)
    w_msg1 = (jax.random.normal(weight_keys[0], (D_IN, D_HID), jnp.float32) * D_IN ** -0.5).astype(jnp.bfloat16)
    w_self1 = (jax.random.normal(weight_keys[1], (D_IN, D_HID), jnp.float32) * D_IN ** -0.5).astype(jnp.bfloat16)
    w_msg2 = (jax.random.normal(weight_keys[2], (D_HID, D_HID), jnp.float32) * D_HID ** -0.5).astype(jnp.bfloat16)
    w_self2 = (jax.random.normal(weight_keys[3], (D_HID, D_HID), jnp.float32) * D_HID ** -0.5).astype(jnp.bfloat16)
    src_local, send_slot, edge_weight, recv_row = draw_graph(part_keys[1])
    return dict(features=features, w_msg1=w_msg1, w_self1=w_self1, w_msg2=w_msg2, w_self2=w_self2, src_local=src_local, send_slot=send_slot, edge_weight=edge_weight, recv_row=recv_row)


def gnn_layer(h_in, w_msg, w_self, src_local, send_slot, edge_weight, recv_ids):
    messages = jnp.dot(h_in, w_msg, preferred_element_type=jnp.float32).astype(jnp.bfloat16)
    msg_blocks = messages.reshape(GRAPH_DEVS, NODES_DEV, D_HID)

    def sender_step(agg_sum, inputs):
        msg_src, src_idx, slot_idx, edge_w, recv_idx = inputs
        weighted = msg_src[src_idx].astype(jnp.float32) * edge_w[:, None]
        partial = jax.ops.segment_sum(weighted, slot_idx, num_segments=GRAPH_DEVS * SLOT_CAP).astype(jnp.bfloat16)
        agg_sum = agg_sum + jax.ops.segment_sum(partial.astype(jnp.float32), recv_idx, num_segments=GRAPH_DEVS * (NODES_DEV + 1))
        return agg_sum, None

    start_sum = jnp.zeros((GRAPH_DEVS * (NODES_DEV + 1), D_HID), jnp.float32)
    agg_sum, _ = lax.scan(sender_step, start_sum, (msg_blocks, src_local, send_slot, edge_weight, recv_ids))
    agg_sum = agg_sum.reshape(GRAPH_DEVS, NODES_DEV + 1, D_HID)[:, :NODES_DEV].reshape(GRAPH_DEVS * NODES_DEV, D_HID)
    self_term = jnp.dot(h_in, w_self, preferred_element_type=jnp.float32)
    return jax.nn.relu(self_term + agg_sum).astype(jnp.bfloat16)


def reference(features, w_msg1, w_self1, w_msg2, w_self2, src_local, send_slot, edge_weight, recv_row):
    dest_base = jnp.arange(GRAPH_DEVS, dtype=jnp.int32)[:, None, None] * (NODES_DEV + 1)
    recv_ids = jnp.transpose(dest_base + recv_row, (1, 0, 2)).reshape(GRAPH_DEVS, GRAPH_DEVS * SLOT_CAP)
    hidden1 = gnn_layer(features, w_msg1, w_self1, src_local, send_slot, edge_weight, recv_ids)
    return gnn_layer(hidden1, w_msg2, w_self2, src_local, send_slot, edge_weight, recv_ids)
```

```python
import functools

import jax
import jax.numpy as jnp
from jax import lax
from jax.experimental import pallas as pl
from jax.experimental.pallas import tpu as pltpu
from jax.sharding import PartitionSpec as P

MESH_ID = pl.DeviceIdType.MESH
BF16, F32, I32 = jnp.bfloat16, jnp.float32, jnp.int32
LANES = 128
PAIR_ROWS = 6
SELF_TILE = 256
ROW_CHUNK = 512
NT = (((1,), (1,)), ((), ()))


def dot(a, b):
    return jnp.dot(a, b, preferred_element_type=F32)


def dot_nt(a, b):
    return lax.dot_general(a, b, NT, preferred_element_type=F32)


def one_hot(count, index_row):
    rows = lax.broadcasted_iota(I32, (count, index_row.shape[1]), 0)
    return jnp.where(rows == index_row, 1.0, 0.0).astype(BF16)


def three_pieces(x):
    high = x.astype(BF16)
    rest = x - high.astype(F32)
    mid = rest.astype(BF16)
    low = (rest - mid.astype(F32)).astype(BF16)
    return high, mid, low


def weighted_sum(values, index_row, count):
    select = one_hot(count, index_row)
    high, mid, low = three_pieces(values)
    return dot_nt(high, select) + dot_nt(mid, select) + dot_nt(low, select)


def prep_kernel(peers, slot_cap, rows_dev, cap, start_ref, flag_ref, key_ref, w_ref, src_ref, rank_ref, wout_ref, meta_ref, keys, weights):
    width = PAIR_ROWS * LANES
    lane = lax.broadcasted_iota(I32, (1, LANES), 1)
    keys[...] = jnp.full(keys.shape, -1, I32)
    weights[...] = jnp.zeros(weights.shape, F32)
    for k in range(peers):
        start = start_ref[k]
        row, shift = start // LANES, start % LANES
        back = (LANES - shift) % LANES
        for ref, out in ((key_ref, keys), (w_ref, weights)):
            turned = [pltpu.roll(ref[row + t], back, 1) for t in range(PAIR_ROWS + 1)]
            for t in range(PAIR_ROWS):
                out[k : k + 1, t * LANES : (t + 1) * LANES] = jnp.where(lane < LANES - shift, turned[t], turned[t + 1])
    key = keys[...]
    lanes = lax.broadcasted_iota(I32, key.shape, 1)
    group = key // rows_dev
    valid = (key >= 0) & (group // slot_cap == lax.broadcasted_iota(I32, key.shape, 0))
    slot = group % slot_cap
    fresh = valid & ((lanes == 0) | (pltpu.roll(group, 1, 1) != group))
    rank = jnp.where(fresh, 1, 0)
    step = 1
    while step < width:
        rank = rank + jnp.where(lanes >= step, pltpu.roll(rank, step, 1), 0)
        step *= 2
    rank = rank - 1
    flag = jnp.maximum(jnp.where(jnp.max(rank) >= cap, 1, 0), flag_ref[0])
    src = jnp.where(valid, key % rows_dev, 0)
    wout = jnp.where(valid, weights[...], 0.0)
    live = jnp.where(valid, rank, -1)
    first = jnp.where(fresh, rank, -1)
    low, high = (slot % 256).astype(F32), (slot // 256).astype(F32)
    sub = lax.broadcasted_iota(I32, (8, width), 0)
    sub_cap = lax.broadcasted_iota(I32, (8, cap), 0)
    for k in range(peers):
        src_ref[k] = src[k : k + 1]
        wout_ref[k] = wout[k : k + 1]
        rank_ref[k] = live[k : k + 1]
        parts = jnp.where(sub == 0, low[k : k + 1], jnp.where(sub == 1, high[k : k + 1], 0.0)).astype(BF16)
        found = dot_nt(parts, one_hot(cap, first[k : k + 1]))
        slots = (found[0:1] + 256.0 * found[1:2]).astype(I32)
        meta_ref[k] = jnp.where(sub_cap == 0, slots, flag)


def gnn_kernel(
    n, groups, cap, feat_ref, w1_ref, w2_ref, src_ref, rank_ref, w_ref, own_src_ref, own_slot_ref, own_w_ref, meta_ref, table_ref,
    out_ref, flag_ref,
    mt, acc, own, send, recv, meta_in, row_ids, flag_own, flag_in,
    send_sem, recv_sem, meta_send_sem, meta_recv_sem, flag_send_sem, flag_recv_sem,
):
    me = lax.axis_index("graph")
    my_group = lax.axis_index("batch")
    peers = n - 1
    rows, hid = feat_ref.shape[0], out_ref.shape[1]
    slot_cap = table_ref.shape[2]
    width = src_ref.shape[2]
    chunks = rows // ROW_CHUNK

    def shift_of(i):
        half = (i + 1) // 2
        return n // 2 + half * (1 - 2 * (i % 2))

    def peer(k):
        return lax.rem(me + k, n)

    def group_peer(j):
        return lax.rem(my_group + j, groups)

    def data_copy(layer, k):
        return pltpu.make_async_remote_copy(
            src_ref=send.at[layer, k - 1], dst_ref=recv.at[layer, k - 1],
            send_sem=send_sem.at[layer, k - 1], recv_sem=recv_sem.at[layer, k - 1],
            device_id={"graph": peer(k)}, device_id_type=MESH_ID,
        )

    def meta_copy(k):
        return pltpu.make_async_remote_copy(
            src_ref=meta_ref.at[k - 1], dst_ref=meta_in.at[k - 1],
            send_sem=meta_send_sem.at[k - 1], recv_sem=meta_recv_sem.at[k - 1],
            device_id={"graph": peer(k)}, device_id_type=MESH_ID,
        )

    def flag_copy(j):
        return pltpu.make_async_remote_copy(
            src_ref=flag_own, dst_ref=flag_in.at[j - 1],
            send_sem=flag_send_sem.at[j - 1], recv_sem=flag_recv_sem.at[j - 1],
            device_id={"batch": group_peer(j)}, device_id_type=MESH_ID,
        )

    barrier = pltpu.get_barrier_semaphore()

    def greet(k, c):
        pl.semaphore_signal(barrier, 1, device_id={"graph": peer(k)}, device_id_type=MESH_ID)
        return c

    def greet_group(j, c):
        pl.semaphore_signal(barrier, 1, device_id={"batch": group_peer(j)}, device_id_type=MESH_ID)
        return c

    lax.fori_loop(1, n, greet, 0)
    lax.fori_loop(1, groups, greet_group, 0)

    def transform(layer, weight_ref, source):
        for c in range(chunks):
            cols = slice(c * ROW_CHUNK, (c + 1) * ROW_CHUNK)
            if layer == 0:
                both = dot_nt(weight_ref[...], source[cols, :])
            else:
                both = dot(weight_ref[...], source[:, cols])
            mt[:, cols] = both[:hid].astype(BF16)
            acc[:, cols] = both[hid:]

    def gather(src_row):
        return dot(mt[...], one_hot(rows, src_row))

    def add_rows(block, ids):
        for c in range(chunks):
            cols = slice(c * ROW_CHUNK, (c + 1) * ROW_CHUNK)
            acc[:, cols] += dot_nt(block, one_hot(ROW_CHUNK, ids - c * ROW_CHUNK))

    def layer_body(layer):
        def send_step(i, c):
            k = shift_of(i)
            total = None
            for t in range(width // SELF_TILE):
                part = slice(t * SELF_TILE, (t + 1) * SELF_TILE)
                values = gather(src_ref[k - 1][:, part]) * w_ref[k - 1][:, part]
                term = weighted_sum(values, rank_ref[k - 1][:, part], cap)
                total = term if total is None else total + term
            send[layer, k - 1] = total.astype(BF16)

            @pl.when(i > 0)
            def _():
                data_copy(layer, shift_of(i - 1)).start()

            return c

        lax.fori_loop(0, peers, send_step, 0)
        data_copy(layer, shift_of(peers - 1)).start()

        own[...] = jnp.zeros(own.shape, F32)

        def own_step(t, c):
            values = gather(own_src_ref[t]) * own_w_ref[t]
            own[...] += weighted_sum(values, own_slot_ref[t], slot_cap)
            return c

        lax.fori_loop(0, own_src_ref.shape[0], own_step, 0)
        add_rows(own[...].astype(BF16), table_ref[me])

        if layer == 0:
            flag_own[...] = jnp.broadcast_to(meta_ref[0][1:2, :LANES], flag_own.shape)

        def recv_step(i, c):
            k = shift_of(i)
            if layer == 0:
                meta_copy(k).wait_recv()
                table = table_ref[lax.rem(me + n - k, n)]
                sub = lax.broadcasted_iota(I32, (8, slot_cap), 0)
                parts = jnp.where(sub == 0, table % 256, jnp.where(sub == 1, table // 256, 0))
                got = meta_in[k - 1]
                found = dot(parts.astype(F32).astype(BF16), one_hot(slot_cap, got[0:1]))
                row_ids[k - 1] = (found[0:1] + 256.0 * found[1:2]).astype(I32)
                flag_own[...] = jnp.maximum(flag_own[...], got[1:2, :LANES])
            data_copy(layer, k).wait_recv()
            add_rows(recv[layer, k - 1], row_ids[k - 1])
            return c

        lax.fori_loop(0, peers, recv_step, 0)

    transform(0, w1_ref, feat_ref)
    pl.semaphore_wait(barrier, n - 1 + groups - 1)

    def start_meta(i, c):
        meta_copy(shift_of(i)).start()
        return c

    lax.fori_loop(0, peers, start_meta, 0)
    layer_body(0)

    hidden = mt
    for c in range(chunks):
        cols = slice(c * ROW_CHUNK, (c + 1) * ROW_CHUNK)
        hidden[:, cols] = jnp.maximum(acc[:, cols], 0.0).astype(BF16)
    transform(1, w2_ref, hidden)

    def start_flag(j, c):
        flag_copy(j).start()
        return c

    lax.fori_loop(1, groups, start_flag, 0)
    layer_body(1)

    for c in range(chunks):
        cols = slice(c * ROW_CHUNK, (c + 1) * ROW_CHUNK)
        out_ref[cols, :] = jnp.transpose(jnp.maximum(acc[:, cols], 0.0)).astype(BF16)

    flag_ref[...] = flag_own[...]

    def end_flag(j, c):
        copy = flag_copy(j)
        copy.wait_recv()
        flag_ref[...] = jnp.maximum(flag_ref[...], flag_in[j - 1])
        copy.wait_send()
        return c

    lax.fori_loop(1, groups, end_flag, 0)

    def end_send(k, c):
        meta_copy(k).wait_send()
        data_copy(0, k).wait_send()
        data_copy(1, k).wait_send()
        return c

    lax.fori_loop(1, n, end_send, 0)


def solution(mesh):
    row_spec = P(("batch", "graph"), None)
    full_spec = P(None, None)
    table_spec = P(("batch", "graph"), None, None)
    n, groups = mesh.shape["graph"], mesh.shape["batch"]

    def plain_layer(h_loc, w_msg, w_self, src_idx, slot_idx, edge_w, recv_idx):
        rows_dev = h_loc.shape[0]
        messages = jnp.dot(h_loc, w_msg, preferred_element_type=F32).astype(BF16)
        weighted = messages[src_idx].astype(F32) * edge_w
        partial = jax.ops.segment_sum(weighted, slot_idx, num_segments=recv_idx.shape[0]).astype(BF16)
        received = lax.all_to_all(partial, "graph", 0, 0, tiled=True)
        agg_sum = jax.ops.segment_sum(received.astype(F32), recv_idx, num_segments=rows_dev + 1)
        self_term = jnp.dot(h_loc, w_self, preferred_element_type=F32)
        return jax.nn.relu(self_term + agg_sum[:rows_dev]).astype(BF16)

    def local_step(features, w_msg1, w_self1, w_msg2, w_self2, src_local, send_slot, edge_weight, recv_row):
        rows_dev, hid = features.shape[0], w_msg1.shape[1]
        slot_cap = recv_row.shape[2]
        edges = src_local.shape[1]
        peers = n - 1
        cap = slot_cap * 3 // 4
        width = PAIR_ROWS * LANES
        own_tiles = edges * 11 // 20 // SELF_TILE
        own_edges = own_tiles * SELF_TILE

        me = lax.axis_index("graph")
        owner, offset = send_slot[0] // slot_cap, send_slot[0] % slot_cap
        rank = lax.rem(owner - me + 2 * n - 1, n)
        key = (rank * slot_cap + offset) * rows_dev + src_local[0]
        counts = jnp.sum((rank[None, :] == jnp.arange(n, dtype=I32)[:, None]).astype(I32), axis=1)
        starts = jnp.cumsum(counts) - counts
        over = jnp.any(counts[:peers] > width) | (counts[peers] > own_edges)
        key, weight = lax.sort((key, edge_weight[0]), num_keys=1, is_stable=False)

        spare = 8 * LANES
        key_rows = jnp.concatenate([key, jnp.full((spare,), -1, I32)]).reshape(-1, 1, LANES)
        weight_rows = jnp.concatenate([weight, jnp.zeros((spare,), F32)]).reshape(-1, 1, LANES)
        vmem, smem = pl.BlockSpec(memory_space=pltpu.VMEM), pl.BlockSpec(memory_space=pltpu.SMEM)
        src, live, wgt, meta = pl.pallas_call(
            functools.partial(prep_kernel, peers, slot_cap, rows_dev, cap),
            out_shape=(
                jax.ShapeDtypeStruct((peers, 1, width), I32),
                jax.ShapeDtypeStruct((peers, 1, width), I32),
                jax.ShapeDtypeStruct((peers, 1, width), F32),
                jax.ShapeDtypeStruct((peers, 8, cap), I32),
            ),
            in_specs=[smem, smem, vmem, vmem],
            out_specs=[vmem] * 4,
            scratch_shapes=[pltpu.VMEM((n, width), I32), pltpu.VMEM((n, width), F32)],
            name="edge_windows",
        )(starts.astype(I32), over.astype(I32).reshape(1), key_rows, weight_rows)

        own_key = key[edges - own_edges :].reshape(own_tiles, 1, SELF_TILE)
        own_group = own_key // rows_dev
        own_slot = jnp.where(own_group // slot_cap == peers, own_group % slot_cap, -1)
        own_src = own_key % rows_dev
        own_w = weight[edges - own_edges :].reshape(own_tiles, 1, SELF_TILE)
        w1 = jnp.concatenate([w_msg1, w_self1], axis=1).T
        w2 = jnp.concatenate([w_msg2, w_self2], axis=1).T
        table = recv_row[0].reshape(n, 1, slot_cap)

        out, flag = pl.pallas_call(
            functools.partial(gnn_kernel, n, groups, cap),
            out_shape=(jax.ShapeDtypeStruct((rows_dev, hid), BF16), jax.ShapeDtypeStruct((8, LANES), I32)),
            in_specs=[vmem] * 11,
            out_specs=[vmem] * 2,
            scratch_shapes=[
                pltpu.VMEM((hid, rows_dev), BF16),
                pltpu.VMEM((hid, rows_dev), F32),
                pltpu.VMEM((hid, slot_cap), F32),
                pltpu.VMEM((2, peers, hid, cap), BF16),
                pltpu.VMEM((2, peers, hid, cap), BF16),
                pltpu.VMEM((peers, 8, cap), I32),
                pltpu.VMEM((peers, 1, cap), I32),
                pltpu.VMEM((8, LANES), I32),
                pltpu.VMEM((max(groups - 1, 1), 8, LANES), I32),
                pltpu.SemaphoreType.DMA((2, peers)),
                pltpu.SemaphoreType.DMA((2, peers)),
                pltpu.SemaphoreType.DMA((peers,)),
                pltpu.SemaphoreType.DMA((peers,)),
                pltpu.SemaphoreType.DMA((max(groups - 1, 1),)),
                pltpu.SemaphoreType.DMA((max(groups - 1, 1),)),
            ],
            compiler_params=pltpu.CompilerParams(collective_id=0, has_side_effects=True, vmem_limit_bytes=56 * 2**20),
            name="gnn_layers",
        )(features, w1, w2, src, live, wgt, own_src, own_slot, own_w, meta, table)

        def plain():
            args = src_local[0], send_slot[0], edge_weight[0][:, None], recv_row[0].reshape(-1)
            hidden = plain_layer(features, w_msg1, w_self1, *args)
            return plain_layer(hidden, w_msg2, w_self2, *args)

        return lax.cond(flag[0, 0] > 0, plain, lambda: out)

    return jax.shard_map(local_step, mesh=mesh, in_specs=(row_spec, full_spec, full_spec, full_spec, full_spec, row_spec, row_spec, row_spec, table_spec), out_specs=row_spec, check_vma=False)
```

```python
import functools

import jax
import jax.numpy as jnp
from jax import lax
from jax.experimental import pallas as pl
from jax.experimental.pallas import tpu as pltpu
from jax.sharding import PartitionSpec as P

MESH_ID = pl.DeviceIdType.MESH
BF16, F32, I32 = jnp.bfloat16, jnp.float32, jnp.int32
LANES = 128
PAIR_ROWS = 6
PAIR_TILE = 256
OWN_ROWS = 4
OWN_SPAN = 512
ROW_CHUNK = 512
NT = (((1,), (1,)), ((), ()))
TN = (((0,), (0,)), ((), ()))


def dot(a, b):
    return jnp.dot(a, b, preferred_element_type=F32)


def dot_nt(a, b):
    return lax.dot_general(a, b, NT, preferred_element_type=F32)


def dot_tn(a, b):
    return lax.dot_general(a, b, TN, preferred_element_type=F32)


def plain_one_hot(count, index_row):
    rows = lax.broadcasted_iota(I32, (count, index_row.shape[1]), 0)
    return jnp.where(rows == index_row, 1.0, 0.0).astype(BF16)


def one_hot(count, index_row):
    width = index_row.shape[1]
    low = plain_one_hot(LANES, index_row & (LANES - 1)).reshape(LANES // 16, 16, width)
    high = jnp.broadcast_to(index_row >> 7, (16, width))
    pieces = [(low * jnp.where(high == i, 1.0, 0.0).astype(BF16)[None]).reshape(LANES, width) for i in range(count // LANES)]
    return jnp.concatenate(pieces, axis=0)


def three_pieces(x):
    high = x.astype(BF16)
    rest = x - high.astype(F32)
    mid = rest.astype(BF16)
    low = (rest - mid.astype(F32)).astype(BF16)
    return high, mid, low


def weighted_sum(values, index_row, count):
    select = one_hot(count, index_row)
    high, mid, low = three_pieces(values)
    return dot_nt(high, select) + dot_nt(mid, select) + dot_nt(low, select)


def prep_kernel(
    peers, slot_cap, rows_dev, cap, count_ref, key_ref, w_ref, table_in_ref,
    src_ref, rank_ref, wout_ref, meta_ref, own_src_ref, own_slot_ref, own_w_ref, table_ref,
    keys, weights, own_keys,
):
    width = PAIR_ROWS * LANES
    slot_bits, row_bits = slot_cap.bit_length() - 1, rows_dev.bit_length() - 1
    edge_rows = key_ref.shape[0]
    own_tiles, own_width = own_src_ref.shape[0], own_src_ref.shape[2]
    ranges = rows_dev // OWN_SPAN
    own_rows = own_tiles // ranges * OWN_ROWS
    lane = lax.broadcasted_iota(I32, (1, LANES), 1)
    keys[...] = jnp.full(keys.shape, -1, I32)
    weights[...] = jnp.zeros(weights.shape, F32)
    start = jnp.int32(0)
    over = jnp.int32(0)
    for k in range(peers + ranges):
        count = count_ref[k]
        kept = PAIR_ROWS if k < peers else own_rows
        over = jnp.maximum(over, jnp.where(count > kept * LANES, 1, 0))
        row, shift = start >> 7, start & (LANES - 1)
        back = (LANES - shift) & (LANES - 1)
        for ref, fill in ((key_ref, -1), (w_ref, 0.0)):
            turned = [pltpu.roll(ref[jnp.minimum(row + t, edge_rows - 1)], back, 1) for t in range(kept + 1)]
            for t in range(kept):
                piece = jnp.where(lane < LANES - shift, turned[t], turned[t + 1])
                piece = jnp.where(lane + t * LANES < count, piece, fill)
                if k < peers:
                    out = keys if ref is key_ref else weights
                    out[k : k + 1, t * LANES : (t + 1) * LANES] = piece
                else:
                    tile, col = divmod((k - peers) * own_rows + t, OWN_ROWS)
                    cols = slice(col * LANES, (col + 1) * LANES)
                    if ref is key_ref:
                        own_keys[tile : tile + 1, cols] = piece
                    else:
                        own_w_ref[tile, :, cols] = piece
        start = start + count
    key = keys[...]
    lanes = lax.broadcasted_iota(I32, key.shape, 1)
    valid = key >= 0
    group = key >> row_bits
    slot = group & (slot_cap - 1)
    fresh = valid & ((lanes == 0) | (pltpu.roll(group, 1, 1) != group))
    rank = jnp.where(fresh, 1, 0)
    step = 1
    while step < width:
        rank = rank + jnp.where(lanes >= step, pltpu.roll(rank, step, 1), 0)
        step *= 2
    rank = rank - 1

    own_key = own_keys[...]
    own_src = jnp.where(own_key >= 0, (own_key >> slot_bits) & (OWN_SPAN - 1), 0)
    own_slot = jnp.where(own_key >= 0, own_key & (slot_cap - 1), -1)
    for t in range(own_tiles):
        own_src_ref[t] = own_src[t : t + 1]
        own_slot_ref[t] = own_slot[t : t + 1]

    flag = jnp.maximum(over, jnp.where(jnp.max(rank) >= cap, 1, 0))
    src = jnp.where(valid, key & (rows_dev - 1), 0)
    live = jnp.where(valid, rank, -1)
    first = jnp.where(fresh, rank, -1)
    low, high = (slot & 255).astype(F32), (slot >> 8).astype(F32)
    sub = lax.broadcasted_iota(I32, (8, width), 0)
    sub_cap = lax.broadcasted_iota(I32, (8, cap), 0)
    for k in range(peers):
        src_ref[k] = src[k : k + 1]
        wout_ref[k] = weights[k : k + 1]
        rank_ref[k] = live[k : k + 1]
        parts = jnp.where(sub == 0, low[k : k + 1], jnp.where(sub == 1, high[k : k + 1], 0.0)).astype(BF16)
        found = dot_nt(parts, one_hot(cap, first[k : k + 1]))
        slots = (found[0:1] + 256.0 * found[1:2]).astype(I32)
        meta_ref[k] = jnp.where(sub_cap == 0, slots, flag)
    for k in range(peers + 1):
        table_ref[k] = table_in_ref[k : k + 1]


def gnn_kernel(
    n, groups, cap, feat_ref, msg1_ref, self1_ref, msg2_ref, self2_ref, src_ref, rank_ref, w_ref, own_src_ref, own_slot_ref, own_w_ref, meta_ref, table_ref,
    out_ref, flag_ref,
    mt, acc, own, send, recv, meta_in, row_ids, flag_own, flag_in,
    send_sem, recv_sem, meta_send_sem, meta_recv_sem, flag_send_sem, flag_recv_sem,
):
    me = lax.axis_index("graph")
    my_group = lax.axis_index("batch")
    peers = n - 1
    rows, hid = out_ref.shape
    slot_cap = table_ref.shape[2]
    width = src_ref.shape[2]
    chunks = rows // ROW_CHUNK

    def shift_of(i):
        half = (i + 1) // 2
        return n // 2 + half * (1 - 2 * (i % 2))

    def peer(k):
        return lax.rem(me + k, n)

    def group_peer(j):
        return lax.rem(my_group + j, groups)

    def data_copy(layer, k):
        return pltpu.make_async_remote_copy(
            src_ref=send.at[layer, k - 1], dst_ref=recv.at[layer, k - 1],
            send_sem=send_sem.at[layer, k - 1], recv_sem=recv_sem.at[layer, k - 1],
            device_id={"graph": peer(k)}, device_id_type=MESH_ID,
        )

    def meta_copy(k):
        return pltpu.make_async_remote_copy(
            src_ref=meta_ref.at[k - 1], dst_ref=meta_in.at[k - 1],
            send_sem=meta_send_sem.at[k - 1], recv_sem=meta_recv_sem.at[k - 1],
            device_id={"graph": peer(k)}, device_id_type=MESH_ID,
        )

    def flag_copy(j):
        return pltpu.make_async_remote_copy(
            src_ref=flag_own, dst_ref=flag_in.at[j - 1],
            send_sem=flag_send_sem.at[j - 1], recv_sem=flag_recv_sem.at[j - 1],
            device_id={"batch": group_peer(j)}, device_id_type=MESH_ID,
        )

    barrier = pltpu.get_barrier_semaphore()

    def greet(k, c):
        pl.semaphore_signal(barrier, 1, device_id={"graph": peer(k)}, device_id_type=MESH_ID)
        return c

    def greet_group(j, c):
        pl.semaphore_signal(barrier, 1, device_id={"batch": group_peer(j)}, device_id_type=MESH_ID)
        return c

    lax.fori_loop(1, n, greet, 0)
    lax.fori_loop(1, groups, greet_group, 0)

    def transform(msg_ref, self_ref, source):
        for c in range(chunks):
            cols = slice(c * ROW_CHUNK, (c + 1) * ROW_CHUNK)
            part = source[:, cols]
            mt[:, cols] = dot_tn(msg_ref[...], part).astype(BF16)
            acc[:, cols] = dot_tn(self_ref[...], part)

    def add_rows(block, ids):
        for c in range(chunks):
            cols = slice(c * ROW_CHUNK, (c + 1) * ROW_CHUNK)
            acc[:, cols] += dot_nt(block, one_hot(ROW_CHUNK, ids - c * ROW_CHUNK))

    def layer_body(layer):
        def send_step(i, c):
            k = shift_of(i)
            total = None
            for t in range(width // PAIR_TILE):
                part = slice(t * PAIR_TILE, (t + 1) * PAIR_TILE)
                values = dot(mt[...], one_hot(rows, src_ref[k - 1][:, part])) * w_ref[k - 1][:, part]
                term = weighted_sum(values, rank_ref[k - 1][:, part], cap)
                total = term if total is None else total + term
            send[layer, k - 1] = total.astype(BF16)

            @pl.when(i > 0)
            def _():
                data_copy(layer, shift_of(i - 1)).start()

            return c

        lax.fori_loop(0, peers, send_step, 0)
        data_copy(layer, shift_of(peers - 1)).start()

        own[...] = jnp.zeros(own.shape, F32)

        def own_step(t, c):
            base = t // (own_src_ref.shape[0] * OWN_SPAN // rows) * OWN_SPAN
            window = mt[:, pl.ds(pl.multiple_of(base, OWN_SPAN), OWN_SPAN)]
            values = dot(window, one_hot(OWN_SPAN, own_src_ref[t])) * own_w_ref[t]
            own[...] += weighted_sum(values, own_slot_ref[t], slot_cap)
            return c

        lax.fori_loop(0, own_src_ref.shape[0], own_step, 0)
        add_rows(own[...].astype(BF16), table_ref[me])

        if layer == 0:
            flag_own[...] = jnp.broadcast_to(meta_ref[0][1:2, :LANES], flag_own.shape)

        def recv_step(i, c):
            k = shift_of(i)
            if layer == 0:
                meta_copy(k).wait_recv()
                table = table_ref[lax.rem(me + n - k, n)]
                sub = lax.broadcasted_iota(I32, (8, slot_cap), 0)
                parts = jnp.where(sub == 0, table & 255, jnp.where(sub == 1, table >> 8, 0))
                got = meta_in[k - 1]
                found = dot(parts.astype(F32).astype(BF16), one_hot(slot_cap, got[0:1]))
                row_ids[k - 1] = (found[0:1] + 256.0 * found[1:2]).astype(I32)
                flag_own[...] = jnp.maximum(flag_own[...], got[1:2, :LANES])
            data_copy(layer, k).wait_recv()
            add_rows(recv[layer, k - 1], row_ids[k - 1])
            return c

        lax.fori_loop(0, peers, recv_step, 0)

    transform(msg1_ref, self1_ref, feat_ref)
    pl.semaphore_wait(barrier, n - 1 + groups - 1)

    def start_meta(i, c):
        meta_copy(shift_of(i)).start()
        return c

    lax.fori_loop(0, peers, start_meta, 0)
    layer_body(0)

    hidden = mt
    for c in range(chunks):
        cols = slice(c * ROW_CHUNK, (c + 1) * ROW_CHUNK)
        hidden[:, cols] = jnp.maximum(acc[:, cols], 0.0).astype(BF16)
    transform(msg2_ref, self2_ref, hidden)

    def start_flag(j, c):
        flag_copy(j).start()
        return c

    lax.fori_loop(1, groups, start_flag, 0)
    layer_body(1)

    for c in range(chunks):
        cols = slice(c * ROW_CHUNK, (c + 1) * ROW_CHUNK)
        out_ref[cols, :] = jnp.transpose(jnp.maximum(acc[:, cols], 0.0)).astype(BF16)

    def end_flag(j, seen):
        copy = flag_copy(j)
        copy.wait_recv()
        seen = jnp.maximum(seen, flag_in[j - 1])
        copy.wait_send()
        return seen

    flag_ref[0] = jnp.max(lax.fori_loop(1, groups, end_flag, flag_own[...]))

    def end_send(k, c):
        meta_copy(k).wait_send()
        data_copy(0, k).wait_send()
        data_copy(1, k).wait_send()
        return c

    lax.fori_loop(1, n, end_send, 0)


def solution(mesh):
    row_spec = P(("batch", "graph"), None)
    full_spec = P(None, None)
    table_spec = P(("batch", "graph"), None, None)
    n, groups = mesh.shape["graph"], mesh.shape["batch"]

    def plain_layer(h_loc, w_msg, w_self, src_idx, slot_idx, edge_w, recv_idx):
        rows_dev = h_loc.shape[0]
        messages = jnp.dot(h_loc, w_msg, preferred_element_type=F32).astype(BF16)
        weighted = messages[src_idx].astype(F32) * edge_w
        partial = jax.ops.segment_sum(weighted, slot_idx, num_segments=recv_idx.shape[0]).astype(BF16)
        received = lax.all_to_all(partial, "graph", 0, 0, tiled=True)
        agg_sum = jax.ops.segment_sum(received.astype(F32), recv_idx, num_segments=rows_dev + 1)
        self_term = jnp.dot(h_loc, w_self, preferred_element_type=F32)
        return jax.nn.relu(self_term + agg_sum[:rows_dev]).astype(BF16)

    def local_step(features, w_msg1, w_self1, w_msg2, w_self2, src_local, send_slot, edge_weight, recv_row):
        rows_dev, hid = features.shape[0], w_msg1.shape[1]
        slot_cap = recv_row.shape[2]
        edges = src_local.shape[1]
        peers = n - 1
        cap = slot_cap * 3 // 4
        width = PAIR_ROWS * LANES
        own_width = OWN_ROWS * LANES
        ranges = rows_dev // OWN_SPAN
        own_tiles = ranges * (edges * 3 // 5 // ranges // own_width)

        me = lax.axis_index("graph")
        slots, sources = send_slot.reshape(-1), src_local.reshape(-1)
        owner, offset = slots // slot_cap, slots % slot_cap
        rank = lax.rem(owner - me + 2 * n - 1, n)
        inner = jnp.where(rank == peers, sources * slot_cap + offset, offset * rows_dev + sources)
        key = rank * (slot_cap * rows_dev) + inner
        bins = jnp.where(rank == peers, peers + sources // OWN_SPAN, rank)
        counts = jnp.sum((bins[None, :] == jnp.arange(peers + ranges, dtype=I32)[:, None]).astype(I32), axis=1)
        key, weight = lax.sort((key, edge_weight.reshape(-1)), num_keys=1, is_stable=False)

        vmem, smem = pl.BlockSpec(memory_space=pltpu.VMEM), pl.BlockSpec(memory_space=pltpu.SMEM)
        pair = lambda dtype: jax.ShapeDtypeStruct((peers, 1, width), dtype)
        own = lambda dtype: jax.ShapeDtypeStruct((own_tiles, 1, own_width), dtype)
        src, live, wgt, meta, own_src, own_slot, own_w, table = pl.pallas_call(
            functools.partial(prep_kernel, peers, slot_cap, rows_dev, cap),
            out_shape=(
                pair(I32), pair(I32), pair(F32), jax.ShapeDtypeStruct((peers, 8, cap), I32), own(I32), own(I32), own(F32),
                jax.ShapeDtypeStruct((n, 1, slot_cap), I32),
            ),
            in_specs=[smem, vmem, vmem, vmem],
            out_specs=[vmem] * 8,
            scratch_shapes=[pltpu.VMEM((n, width), I32), pltpu.VMEM((n, width), F32), pltpu.VMEM((own_tiles, own_width), I32)],
            name="edge_windows",
        )(counts, key.reshape(-1, 1, LANES), weight.reshape(-1, 1, LANES), recv_row[0])

        out, flag = pl.pallas_call(
            functools.partial(gnn_kernel, n, groups, cap),
            out_shape=(jax.ShapeDtypeStruct((rows_dev, hid), BF16), jax.ShapeDtypeStruct((1,), I32)),
            in_specs=[vmem] * 13,
            out_specs=[vmem, smem],
            scratch_shapes=[
                pltpu.VMEM((hid, rows_dev), BF16),
                pltpu.VMEM((hid, rows_dev), F32),
                pltpu.VMEM((hid, slot_cap), F32),
                pltpu.VMEM((2, peers, hid, cap), BF16),
                pltpu.VMEM((2, peers, hid, cap), BF16),
                pltpu.VMEM((peers, 8, cap), I32),
                pltpu.VMEM((peers, 1, cap), I32),
                pltpu.VMEM((8, LANES), I32),
                pltpu.VMEM((max(groups - 1, 1), 8, LANES), I32),
                pltpu.SemaphoreType.DMA((2, peers)),
                pltpu.SemaphoreType.DMA((2, peers)),
                pltpu.SemaphoreType.DMA((peers,)),
                pltpu.SemaphoreType.DMA((peers,)),
                pltpu.SemaphoreType.DMA((max(groups - 1, 1),)),
                pltpu.SemaphoreType.DMA((max(groups - 1, 1),)),
            ],
            compiler_params=pltpu.CompilerParams(collective_id=0, has_side_effects=True, vmem_limit_bytes=56 * 2**20),
            name="gnn_layers",
        )(features.T, w_msg1, w_self1, w_msg2, w_self2, src, live, wgt, own_src, own_slot, own_w, meta, table)

        def plain():
            args = src_local[0], send_slot[0], edge_weight[0][:, None], recv_row[0].reshape(-1)
            extra = features.shape[1] - hid
            grow = lambda w: jnp.pad(w, ((0, extra), (0, 0)))
            msg, own_part = jnp.stack([w_msg1, grow(w_msg2)]), jnp.stack([w_self1, grow(w_self2)])

            def step(h, weights):
                return jnp.pad(plain_layer(h, *weights, *args), ((0, 0), (0, extra))), None

            hidden, _ = lax.scan(step, features, (msg, own_part))
            return hidden[:, :hid]

        return lax.cond(flag[0] > 0, plain, lambda: out)

    return jax.shard_map(local_step, mesh=mesh, in_specs=(row_spec, full_spec, full_spec, full_spec, full_spec, row_spec, row_spec, row_spec, table_spec), out_specs=row_spec, check_vma=False)
```

```python
import functools

import jax
import jax.numpy as jnp
from jax import lax
from jax.experimental import pallas as pl
from jax.experimental.pallas import tpu as pltpu
from jax.sharding import PartitionSpec as P

MESH_ID = pl.DeviceIdType.MESH
BF16, F32, I32 = jnp.bfloat16, jnp.float32, jnp.int32
LANES = 128
PAIR_ROWS = 6
PAIR_TILE = 256
OWN_ROWS = 4
OWN_SPAN = 512
ROW_CHUNK = 512
NT = (((1,), (1,)), ((), ()))
TN = (((0,), (0,)), ((), ()))


def dot(a, b):
    return jnp.dot(a, b, preferred_element_type=F32)


def dot_nt(a, b):
    return lax.dot_general(a, b, NT, preferred_element_type=F32)


def dot_tn(a, b):
    return lax.dot_general(a, b, TN, preferred_element_type=F32)


def plain_one_hot(count, index_row):
    rows = lax.broadcasted_iota(I32, (count, index_row.shape[1]), 0)
    return jnp.where(rows == index_row, 1.0, 0.0).astype(BF16)


def one_hot(count, index_row):
    width = index_row.shape[1]
    low = plain_one_hot(LANES, index_row & (LANES - 1)).reshape(LANES // 16, 16, width)
    high = jnp.broadcast_to(index_row >> 7, (16, width))
    pieces = [(low * jnp.where(high == i, 1.0, 0.0).astype(BF16)[None]).reshape(LANES, width) for i in range(count // LANES)]
    return jnp.concatenate(pieces, axis=0)


def three_pieces(x):
    high = x.astype(BF16)
    rest = x - high.astype(F32)
    mid = rest.astype(BF16)
    low = (rest - mid.astype(F32)).astype(BF16)
    return high, mid, low


def weighted_sum(values, index_row, count):
    select = one_hot(count, index_row)
    high, mid, low = three_pieces(values)
    return dot_nt(select, high) + dot_nt(select, mid) + dot_nt(select, low)


def prep_kernel(
    peers, slot_cap, rows_dev, cap, key2_ref, key_ref, w_ref, table_in_ref,
    src_ref, rank_ref, wout_ref, meta_ref, own_src_ref, own_slot_ref, own_w_ref, table_ref,
    keys, weights, own_keys,
):
    width = PAIR_ROWS * LANES
    slot_bits, row_bits = slot_cap.bit_length() - 1, rows_dev.bit_length() - 1
    edge_rows = key_ref.shape[0]
    own_tiles, own_width = own_src_ref.shape[0], own_src_ref.shape[2]
    ranges = rows_dev // OWN_SPAN
    own_rows = own_tiles // ranges * OWN_ROWS
    lane = lax.broadcasted_iota(I32, (1, LANES), 1)
    keys[...] = jnp.full(keys.shape, -1, I32)
    weights[...] = jnp.zeros(weights.shape, F32)
    all_keys = key2_ref[...]
    bounds = [k * slot_cap * rows_dev for k in range(1, peers + 1)]
    bounds += [(peers * rows_dev + r * OWN_SPAN) * slot_cap for r in range(1, ranges)]
    starts = [jnp.int32(0)] + [jnp.sum(jnp.where(all_keys < bound, 1, 0)) for bound in bounds] + [jnp.int32(edge_rows * LANES)]
    over = jnp.int32(0)
    for k in range(peers + ranges):
        start, count = starts[k], starts[k + 1] - starts[k]
        kept = PAIR_ROWS if k < peers else own_rows
        over = jnp.maximum(over, jnp.where(count > kept * LANES, 1, 0))
        row, shift = start >> 7, start & (LANES - 1)
        back = (LANES - shift) & (LANES - 1)
        for ref, fill in ((key_ref, -1), (w_ref, 0.0)):
            turned = [pltpu.roll(ref[jnp.minimum(row + t, edge_rows - 1)], back, 1) for t in range(kept + 1)]
            for t in range(kept):
                piece = jnp.where(lane < LANES - shift, turned[t], turned[t + 1])
                piece = jnp.where(lane + t * LANES < count, piece, fill)
                if k < peers:
                    out = keys if ref is key_ref else weights
                    out[k : k + 1, t * LANES : (t + 1) * LANES] = piece
                else:
                    tile, col = divmod((k - peers) * own_rows + t, OWN_ROWS)
                    cols = slice(col * LANES, (col + 1) * LANES)
                    if ref is key_ref:
                        own_keys[tile : tile + 1, cols] = piece
                    else:
                        own_w_ref[tile, :, cols] = piece
    key = keys[...]
    lanes = lax.broadcasted_iota(I32, key.shape, 1)
    valid = key >= 0
    group = key >> row_bits
    slot = group & (slot_cap - 1)
    fresh = valid & ((lanes == 0) | (pltpu.roll(group, 1, 1) != group))
    rank = jnp.where(fresh, 1, 0)
    step = 1
    while step < width:
        rank = rank + jnp.where(lanes >= step, pltpu.roll(rank, step, 1), 0)
        step *= 2
    rank = rank - 1

    own_key = own_keys[...]
    own_src = jnp.where(own_key >= 0, (own_key >> slot_bits) & (OWN_SPAN - 1), 0)
    own_slot = jnp.where(own_key >= 0, own_key & (slot_cap - 1), -1)
    for t in range(own_tiles):
        own_src_ref[t] = own_src[t : t + 1]
        own_slot_ref[t] = own_slot[t : t + 1]

    flag = jnp.maximum(over, jnp.where(jnp.max(rank) >= cap, 1, 0))
    src = jnp.where(valid, key & (rows_dev - 1), 0)
    live = jnp.where(valid, rank, -1)
    first = jnp.where(fresh, rank, -1)
    lanes_cap = meta_ref.shape[2]
    sub = lax.broadcasted_iota(I32, (8, width), 0)
    sub_cap = lax.broadcasted_iota(I32, (8, lanes_cap), 0)
    low, high = (slot & 255).astype(F32), (slot >> 8).astype(F32)
    for k in range(peers):
        src_ref[k] = src[k : k + 1]
        wout_ref[k] = weights[k : k + 1]
        rank_ref[k] = live[k : k + 1]
        parts = jnp.where(sub == 0, low[k : k + 1], jnp.where(sub == 1, high[k : k + 1], 0.0)).astype(BF16)
        found = dot_nt(parts, one_hot(lanes_cap, first[k : k + 1]))
        listed = (found[0:1] + 256.0 * found[1:2]).astype(I32)
        meta_ref[k] = jnp.where(sub_cap == 0, listed, flag)
    for k in range(peers + 1):
        table_ref[k] = table_in_ref[k : k + 1]


def gnn_kernel(
    n, groups, cap, feat_ref, msg1_ref, self1_ref, msg2_ref, self2_ref, src_ref, rank_ref, w_ref, own_src_ref, own_slot_ref, own_w_ref, meta_ref, table_ref,
    out_ref, flag_ref,
    mt, hidden, acc, own, send, recv, meta_in, row_ids, flag_own, flag_in,
    send_sem, recv_sem, meta_send_sem, meta_recv_sem, flag_send_sem, flag_recv_sem,
):
    me = lax.axis_index("graph")
    my_group = lax.axis_index("batch")
    peers = n - 1
    rows, hid = out_ref.shape
    slot_cap = table_ref.shape[2]
    width = src_ref.shape[2]
    chunks = rows // ROW_CHUNK

    def shift_of(i):
        half = (i + 1) // 2
        return n // 2 + half * (1 - 2 * (i % 2))

    def peer(k):
        return lax.rem(me + k, n)

    def group_peer(j):
        return lax.rem(my_group + j, groups)

    def data_copy(layer, k):
        return pltpu.make_async_remote_copy(
            src_ref=send.at[layer, k - 1, pl.ds(0, cap)], dst_ref=recv.at[layer, k - 1, pl.ds(0, cap)],
            send_sem=send_sem.at[layer, k - 1], recv_sem=recv_sem.at[layer, k - 1],
            device_id={"graph": peer(k)}, device_id_type=MESH_ID,
        )

    def meta_copy(k):
        return pltpu.make_async_remote_copy(
            src_ref=meta_ref.at[k - 1], dst_ref=meta_in.at[k - 1],
            send_sem=meta_send_sem.at[k - 1], recv_sem=meta_recv_sem.at[k - 1],
            device_id={"graph": peer(k)}, device_id_type=MESH_ID,
        )

    def flag_copy(j):
        return pltpu.make_async_remote_copy(
            src_ref=flag_own, dst_ref=flag_in.at[j - 1],
            send_sem=flag_send_sem.at[j - 1], recv_sem=flag_recv_sem.at[j - 1],
            device_id={"batch": group_peer(j)}, device_id_type=MESH_ID,
        )

    barrier = pltpu.get_barrier_semaphore()

    def greet(k, c):
        pl.semaphore_signal(barrier, 1, device_id={"graph": peer(k)}, device_id_type=MESH_ID)
        return c

    def greet_group(j, c):
        pl.semaphore_signal(barrier, 1, device_id={"batch": group_peer(j)}, device_id_type=MESH_ID)
        return c

    lax.fori_loop(1, n, greet, 0)
    lax.fori_loop(1, groups, greet_group, 0)

    def add_rows(block, ids):
        for c in range(chunks):
            part = slice(c * ROW_CHUNK, (c + 1) * ROW_CHUNK)
            acc[part] += dot(one_hot(ROW_CHUNK, ids - c * ROW_CHUNK), block)

    def layer_body(layer):
        def pair_sum(k, between):
            total = None
            for t in range(width // PAIR_TILE):
                part = slice(t * PAIR_TILE, (t + 1) * PAIR_TILE)
                values = dot(mt[...], one_hot(rows, src_ref[k - 1][:, part])) * w_ref[k - 1][:, part]
                term = weighted_sum(values, rank_ref[k - 1][:, part], send.shape[2])
                total = term if total is None else total + term
                if t == 0:
                    between()
            send[layer, k - 1] = total.astype(BF16)

        def send_step(i, c):
            pair_sum(shift_of(i), lambda: data_copy(layer, shift_of(i - 1)).start())
            return c

        pair_sum(shift_of(0), lambda: None)
        lax.fori_loop(1, peers, send_step, 0)

        for c in range(chunks):
            part = slice(c * ROW_CHUNK, (c + 1) * ROW_CHUNK)
            if layer == 0:
                acc[part] = dot_tn(feat_ref[:, part], self1_ref[...])
            else:
                acc[part] = dot(hidden[part], self2_ref[...])
            if c == 0:
                data_copy(layer, shift_of(peers - 1)).start()

        own[...] = jnp.zeros(own.shape, F32)

        def own_step(t, c):
            base = t // (own_src_ref.shape[0] * OWN_SPAN // rows) * OWN_SPAN
            window = mt[:, pl.ds(pl.multiple_of(base, OWN_SPAN), OWN_SPAN)]
            values = dot(window, one_hot(OWN_SPAN, own_src_ref[t])) * own_w_ref[t]
            own[...] += weighted_sum(values, own_slot_ref[t], slot_cap)
            return c

        lax.fori_loop(0, own_src_ref.shape[0], own_step, 0)
        add_rows(own[...].astype(BF16), table_ref[me])

        if layer == 0:
            flag_own[...] = jnp.broadcast_to(meta_ref[0][1:2, :LANES], flag_own.shape)

        def recv_step(i, c):
            k = shift_of(i)
            if layer == 0:
                meta_copy(k).wait_recv()
                table = table_ref[lax.rem(me + n - k, n)]
                sub = lax.broadcasted_iota(I32, (8, slot_cap), 0)
                parts = jnp.where(sub == 0, table & 255, jnp.where(sub == 1, table >> 8, 0))
                got = meta_in[k - 1]
                found = dot(parts.astype(F32).astype(BF16), one_hot(slot_cap, got[0:1]))
                row_ids[k - 1] = (found[0:1] + 256.0 * found[1:2]).astype(I32)
                flag_own[...] = jnp.maximum(flag_own[...], got[1:2, :LANES])
            data_copy(layer, k).wait_recv()
            add_rows(recv[layer, k - 1], row_ids[k - 1])
            return c

        lax.fori_loop(0, peers, recv_step, 0)

    spare = recv.shape[2] - cap
    recv[:, :, cap:, :] = jnp.zeros((2, peers, spare, hid), BF16)
    for c in range(chunks):
        part = slice(c * ROW_CHUNK, (c + 1) * ROW_CHUNK)
        mt[:, part] = dot_tn(msg1_ref[...], feat_ref[:, part]).astype(BF16)
    pl.semaphore_wait(barrier, n - 1 + groups - 1)

    def start_meta(i, c):
        meta_copy(shift_of(i)).start()
        return c

    lax.fori_loop(0, peers, start_meta, 0)
    layer_body(0)

    for c in range(chunks):
        part = slice(c * ROW_CHUNK, (c + 1) * ROW_CHUNK)
        hidden[part] = jnp.maximum(acc[part], 0.0).astype(BF16)
        mt[:, part] = lax.dot_general(msg2_ref[...], hidden[part], (((0,), (1,)), ((), ())), preferred_element_type=F32).astype(BF16)

    def start_flag(j, c):
        flag_copy(j).start()
        return c

    lax.fori_loop(1, groups, start_flag, 0)
    layer_body(1)

    out_ref[...] = acc[...].astype(BF16)

    def end_flag(j, seen):
        copy = flag_copy(j)
        copy.wait_recv()
        seen = jnp.maximum(seen, flag_in[j - 1])
        copy.wait_send()
        return seen

    flag_ref[0] = jnp.max(lax.fori_loop(1, groups, end_flag, flag_own[...]))

    def end_send(k, c):
        meta_copy(k).wait_send()
        data_copy(0, k).wait_send()
        data_copy(1, k).wait_send()
        return c

    lax.fori_loop(1, n, end_send, 0)


def solution(mesh):
    row_spec = P(("batch", "graph"), None)
    full_spec = P(None, None)
    table_spec = P(("batch", "graph"), None, None)
    n, groups = mesh.shape["graph"], mesh.shape["batch"]

    def plain_layer(h_loc, w_msg, w_self, src_idx, slot_idx, edge_w, recv_idx):
        rows_dev = h_loc.shape[0]
        messages = jnp.dot(h_loc, w_msg, preferred_element_type=F32).astype(BF16)
        weighted = messages[src_idx].astype(F32) * edge_w
        partial = jax.ops.segment_sum(weighted, slot_idx, num_segments=recv_idx.shape[0]).astype(BF16)
        received = lax.all_to_all(partial, "graph", 0, 0, tiled=True)
        agg_sum = jax.ops.segment_sum(received.astype(F32), recv_idx, num_segments=rows_dev + 1)
        self_term = jnp.dot(h_loc, w_self, preferred_element_type=F32)
        return jax.nn.relu(self_term + agg_sum[:rows_dev]).astype(BF16)

    def local_step(features, w_msg1, w_self1, w_msg2, w_self2, src_local, send_slot, edge_weight, recv_row):
        rows_dev, hid = features.shape[0], w_msg1.shape[1]
        slot_cap = recv_row.shape[2]
        edges = src_local.shape[1]
        peers = n - 1
        cap, lanes_cap = slot_cap * 23 // 32, slot_cap * 3 // 4
        width = PAIR_ROWS * LANES
        own_width = OWN_ROWS * LANES
        ranges = rows_dev // OWN_SPAN
        own_tiles = ranges * (edges * 3 // 5 // ranges // own_width)

        me = lax.axis_index("graph")
        slots, sources = send_slot.reshape(-1), src_local.reshape(-1)
        owner, offset = slots // slot_cap, slots % slot_cap
        rank = lax.rem(owner - me + 2 * n - 1, n)
        inner = jnp.where(rank == peers, sources * slot_cap + offset, offset * rows_dev + sources)
        key = rank * (slot_cap * rows_dev) + inner
        key, weight = lax.sort((key, edge_weight.reshape(-1)), num_keys=1, is_stable=False)

        vmem, smem = pl.BlockSpec(memory_space=pltpu.VMEM), pl.BlockSpec(memory_space=pltpu.SMEM)
        pair = lambda dtype: jax.ShapeDtypeStruct((peers, 1, width), dtype)
        own = lambda dtype: jax.ShapeDtypeStruct((own_tiles, 1, own_width), dtype)
        src, live, wgt, meta, own_src, own_slot, own_w, table = pl.pallas_call(
            functools.partial(prep_kernel, peers, slot_cap, rows_dev, cap),
            out_shape=(
                pair(I32), pair(I32), pair(F32), jax.ShapeDtypeStruct((peers, 8, lanes_cap), I32), own(I32), own(I32), own(F32),
                jax.ShapeDtypeStruct((n, 1, slot_cap), I32),
            ),
            in_specs=[vmem] * 4,
            out_specs=[vmem] * 8,
            scratch_shapes=[pltpu.VMEM((n, width), I32), pltpu.VMEM((n, width), F32), pltpu.VMEM((own_tiles, own_width), I32)],
            name="edge_windows",
        )(key.reshape(-1, LANES), key.reshape(-1, 1, LANES), weight.reshape(-1, 1, LANES), recv_row[0])

        out, flag = pl.pallas_call(
            functools.partial(gnn_kernel, n, groups, cap),
            out_shape=(jax.ShapeDtypeStruct((rows_dev, hid), BF16), jax.ShapeDtypeStruct((1,), I32)),
            in_specs=[vmem] * 13,
            out_specs=[vmem, smem],
            scratch_shapes=[
                pltpu.VMEM((hid, rows_dev), BF16),
                pltpu.VMEM((rows_dev, hid), BF16),
                pltpu.VMEM((rows_dev, hid), F32),
                pltpu.VMEM((slot_cap, hid), F32),
                pltpu.VMEM((2, peers, lanes_cap, hid), BF16),
                pltpu.VMEM((2, peers, lanes_cap, hid), BF16),
                pltpu.VMEM((peers, 8, lanes_cap), I32),
                pltpu.VMEM((peers, 1, lanes_cap), I32),
                pltpu.VMEM((8, LANES), I32),
                pltpu.VMEM((max(groups - 1, 1), 8, LANES), I32),
                pltpu.SemaphoreType.DMA((2, peers)),
                pltpu.SemaphoreType.DMA((2, peers)),
                pltpu.SemaphoreType.DMA((peers,)),
                pltpu.SemaphoreType.DMA((peers,)),
                pltpu.SemaphoreType.DMA((max(groups - 1, 1),)),
                pltpu.SemaphoreType.DMA((max(groups - 1, 1),)),
            ],
            compiler_params=pltpu.CompilerParams(collective_id=0, has_side_effects=True, vmem_limit_bytes=56 * 2**20),
            name="gnn_layers",
        )(features.T, w_msg1, w_self1, w_msg2, w_self2, src, live, wgt, own_src, own_slot, own_w, meta, table)

        def plain():
            args = src_local[0], send_slot[0], edge_weight[0][:, None], recv_row[0].reshape(-1)
            extra = features.shape[1] - hid
            grow = lambda w: jnp.pad(w, ((0, extra), (0, 0)))
            msg, own_part = jnp.stack([w_msg1, grow(w_msg2)]), jnp.stack([w_self1, grow(w_self2)])

            def step(h, weights):
                return jnp.pad(plain_layer(h, *weights, *args), ((0, 0), (0, extra))), None

            hidden, _ = lax.scan(step, features, (msg, own_part))
            return hidden[:, :hid]

        return jnp.maximum(lax.cond(flag[0] > 0, plain, lambda: out), 0)

    return jax.shard_map(local_step, mesh=mesh, in_specs=(row_spec, full_spec, full_spec, full_spec, full_spec, row_spec, row_spec, row_spec, table_spec), out_specs=row_spec, check_vma=False)
```

```python
import functools

import jax
import jax.numpy as jnp
from jax import lax
from jax.experimental import pallas as pl
from jax.experimental.pallas import tpu as pltpu
from jax.sharding import PartitionSpec as P

MESH_ID = pl.DeviceIdType.MESH
BF16, F32, I32 = jnp.bfloat16, jnp.float32, jnp.int32
LANES = 128
PAIR_ROWS = 6
PAIR_TILE = 256
OWN_ROWS = 4
OWN_SPAN = 512
ROW_CHUNK = 512
NT = (((1,), (1,)), ((), ()))
TN = (((0,), (0,)), ((), ()))


def dot(a, b):
    return jnp.dot(a, b, preferred_element_type=F32)


def dot_nt(a, b):
    return lax.dot_general(a, b, NT, preferred_element_type=F32)


def dot_tn(a, b):
    return lax.dot_general(a, b, TN, preferred_element_type=F32)


def plain_one_hot(count, index_row):
    rows = lax.broadcasted_iota(I32, (count, index_row.shape[1]), 0)
    return jnp.where(rows == index_row, 1.0, 0.0).astype(BF16)


def one_hot(count, index_row):
    width = index_row.shape[1]
    low = plain_one_hot(LANES, index_row & (LANES - 1)).reshape(LANES // 16, 16, width)
    high = jnp.broadcast_to(index_row >> 7, (16, width))
    pieces = [(low * jnp.where(high == i, 1.0, 0.0).astype(BF16)[None]).reshape(LANES, width) for i in range(count // LANES)]
    return jnp.concatenate(pieces, axis=0)


def three_pieces(x):
    high = x.astype(BF16)
    rest = x - high.astype(F32)
    mid = rest.astype(BF16)
    low = (rest - mid.astype(F32)).astype(BF16)
    return high, mid, low


def weighted_sum(values, index_row, count):
    select = one_hot(count, index_row)
    high, mid, low = three_pieces(values)
    return dot_nt(select, high) + dot_nt(select, mid) + dot_nt(select, low)


def weighted_sum_columns(values, index_row, count):
    select = one_hot(count, index_row)
    high, mid, low = three_pieces(values)
    return dot_nt(high, select) + dot_nt(mid, select) + dot_nt(low, select)


def prep_kernel(
    peers, slot_cap, rows_dev, cap, key2_ref, key_ref, w_ref, table_in_ref,
    src_ref, rank_ref, wout_ref, meta_ref, own_src_ref, own_slot_ref, own_w_ref, table_ref,
    keys, weights, own_keys,
):
    width = PAIR_ROWS * LANES
    slot_bits, row_bits = slot_cap.bit_length() - 1, rows_dev.bit_length() - 1
    edge_rows = key_ref.shape[0]
    own_tiles, own_width = own_src_ref.shape[0], own_src_ref.shape[2]
    ranges = rows_dev // OWN_SPAN
    own_rows = own_tiles // ranges * OWN_ROWS
    lane = lax.broadcasted_iota(I32, (1, LANES), 1)
    keys[...] = jnp.full(keys.shape, -1, I32)
    weights[...] = jnp.zeros(weights.shape, F32)
    all_keys = key2_ref[...]
    bounds = [k * slot_cap * rows_dev for k in range(1, peers + 1)]
    bounds += [(peers * rows_dev + r * OWN_SPAN) * slot_cap for r in range(1, ranges)]
    starts = [jnp.int32(0)] + [jnp.sum(jnp.where(all_keys < bound, 1, 0)) for bound in bounds] + [jnp.int32(edge_rows * LANES)]
    over = jnp.int32(0)
    for k in range(peers + ranges):
        start, count = starts[k], starts[k + 1] - starts[k]
        kept = PAIR_ROWS if k < peers else own_rows
        over = jnp.maximum(over, jnp.where(count > kept * LANES, 1, 0))
        row, shift = start >> 7, start & (LANES - 1)
        back = (LANES - shift) & (LANES - 1)
        for ref, fill in ((key_ref, -1), (w_ref, 0.0)):
            turned = [pltpu.roll(ref[jnp.minimum(row + t, edge_rows - 1)], back, 1) for t in range(kept + 1)]
            for t in range(kept):
                piece = jnp.where(lane < LANES - shift, turned[t], turned[t + 1])
                piece = jnp.where(lane + t * LANES < count, piece, fill)
                if k < peers:
                    out = keys if ref is key_ref else weights
                    out[k : k + 1, t * LANES : (t + 1) * LANES] = piece
                else:
                    tile, col = divmod((k - peers) * own_rows + t, OWN_ROWS)
                    cols = slice(col * LANES, (col + 1) * LANES)
                    if ref is key_ref:
                        own_keys[tile : tile + 1, cols] = piece
                    else:
                        own_w_ref[tile, :, cols] = piece
    key = keys[...]
    lanes = lax.broadcasted_iota(I32, key.shape, 1)
    valid = key >= 0
    group = key >> row_bits
    slot = group & (slot_cap - 1)
    fresh = valid & ((lanes == 0) | (pltpu.roll(group, 1, 1) != group))
    rank = jnp.where(fresh, 1, 0)
    step = 1
    while step < width:
        rank = rank + jnp.where(lanes >= step, pltpu.roll(rank, step, 1), 0)
        step *= 2
    rank = rank - 1

    own_key = own_keys[...]
    own_src = jnp.where(own_key >= 0, (own_key >> slot_bits) & (OWN_SPAN - 1), 0)
    own_slot = jnp.where(own_key >= 0, own_key & (slot_cap - 1), -1)
    for t in range(own_tiles):
        own_src_ref[t] = own_src[t : t + 1]
        own_slot_ref[t] = own_slot[t : t + 1]

    flag = jnp.maximum(over, jnp.where(jnp.max(rank) >= cap, 1, 0))
    src = jnp.where(valid, key & (rows_dev - 1), 0)
    live = jnp.where(valid, rank, -1)
    first = jnp.where(fresh, rank, -1)
    lanes_cap = meta_ref.shape[2]
    sub = lax.broadcasted_iota(I32, (8, width), 0)
    sub_cap = lax.broadcasted_iota(I32, (8, lanes_cap), 0)
    low, high = (slot & 255).astype(F32), (slot >> 8).astype(F32)
    for k in range(peers):
        src_ref[k] = src[k : k + 1]
        wout_ref[k] = weights[k : k + 1]
        rank_ref[k] = live[k : k + 1]
        parts = jnp.where(sub == 0, low[k : k + 1], jnp.where(sub == 1, high[k : k + 1], 0.0)).astype(BF16)
        found = dot_nt(parts, one_hot(lanes_cap, first[k : k + 1]))
        listed = (found[0:1] + 256.0 * found[1:2]).astype(I32)
        meta_ref[k] = jnp.where(sub_cap == 0, listed, flag)
    for k in range(peers + 1):
        table_ref[k] = table_in_ref[k : k + 1]


def gnn_kernel(
    n, groups, cap, feat_ref, msg1_ref, self1_ref, msg2_ref, self2_ref, src_ref, rank_ref, w_ref, own_src_ref, own_slot_ref, own_w_ref, meta_ref, table_ref,
    out_ref, flag_ref,
    mt, hidden, acc, own, send, recv, meta_in, row_ids, flag_own, flag_in,
    send_sem, recv_sem, meta_send_sem, meta_recv_sem, flag_send_sem, flag_recv_sem,
):
    me = lax.axis_index("graph")
    my_group = lax.axis_index("batch")
    peers = n - 1
    rows, hid = out_ref.shape
    slot_cap = table_ref.shape[2]
    width = src_ref.shape[2]
    chunks = rows // ROW_CHUNK

    def shift_of(i):
        half = (i + 1) // 2
        return n // 2 + half * (1 - 2 * (i % 2))

    def peer(k):
        return lax.rem(me + k, n)

    def group_peer(j):
        return lax.rem(my_group + j, groups)

    def data_copy(layer, k):
        return pltpu.make_async_remote_copy(
            src_ref=send.at[layer, k - 1, pl.ds(0, cap)], dst_ref=recv.at[layer, k - 1, pl.ds(0, cap)],
            send_sem=send_sem.at[layer, k - 1], recv_sem=recv_sem.at[layer, k - 1],
            device_id={"graph": peer(k)}, device_id_type=MESH_ID,
        )

    def meta_copy(k):
        return pltpu.make_async_remote_copy(
            src_ref=meta_ref.at[k - 1], dst_ref=meta_in.at[k - 1],
            send_sem=meta_send_sem.at[k - 1], recv_sem=meta_recv_sem.at[k - 1],
            device_id={"graph": peer(k)}, device_id_type=MESH_ID,
        )

    def flag_copy(j):
        return pltpu.make_async_remote_copy(
            src_ref=flag_own, dst_ref=flag_in.at[j - 1],
            send_sem=flag_send_sem.at[j - 1], recv_sem=flag_recv_sem.at[j - 1],
            device_id={"batch": group_peer(j)}, device_id_type=MESH_ID,
        )

    barrier = pltpu.get_barrier_semaphore()

    def greet(k, c):
        pl.semaphore_signal(barrier, 1, device_id={"graph": peer(k)}, device_id_type=MESH_ID)
        return c

    def greet_group(j, c):
        pl.semaphore_signal(barrier, 1, device_id={"batch": group_peer(j)}, device_id_type=MESH_ID)
        return c

    lax.fori_loop(1, n, greet, 0)
    lax.fori_loop(1, groups, greet_group, 0)

    def add_rows(block, ids):
        for c in range(chunks):
            part = slice(c * ROW_CHUNK, (c + 1) * ROW_CHUNK)
            acc[part] += dot(one_hot(ROW_CHUNK, ids - c * ROW_CHUNK), block)

    def layer_body(layer):
        def pair_sum(k, between):
            total = None
            for t in range(width // PAIR_TILE):
                part = slice(t * PAIR_TILE, (t + 1) * PAIR_TILE)
                values = dot(mt[...], one_hot(rows, src_ref[k - 1][:, part])) * w_ref[k - 1][:, part]
                term = weighted_sum(values, rank_ref[k - 1][:, part], send.shape[2])
                total = term if total is None else total + term
                if t == 0:
                    between()
            send[layer, k - 1] = total.astype(BF16)

        def send_step(i, c):
            pair_sum(shift_of(i), lambda: data_copy(layer, shift_of(i - 1)).start())
            return c

        pair_sum(shift_of(0), lambda: None)
        lax.fori_loop(1, peers, send_step, 0)

        for c in range(chunks):
            part = slice(c * ROW_CHUNK, (c + 1) * ROW_CHUNK)
            if layer == 0:
                acc[part] = dot_tn(feat_ref[:, part], self1_ref[...])
            else:
                acc[part] = dot(hidden[part], self2_ref[...])
            if c == 0:
                data_copy(layer, shift_of(peers - 1)).start()

        own[...] = jnp.zeros(own.shape, F32)

        def own_step(t, c):
            base = t // (own_src_ref.shape[0] * OWN_SPAN // rows) * OWN_SPAN
            window = mt[:, pl.ds(pl.multiple_of(base, OWN_SPAN), OWN_SPAN)]
            values = dot(window, one_hot(OWN_SPAN, own_src_ref[t])) * own_w_ref[t]
            own[...] += weighted_sum_columns(values, own_slot_ref[t], slot_cap)
            return c

        lax.fori_loop(0, own_src_ref.shape[0], own_step, 0)
        add_rows(jnp.transpose(own[...]).astype(BF16), table_ref[me])

        if layer == 0:
            flag_own[...] = jnp.broadcast_to(meta_ref[0][1:2, :LANES], flag_own.shape)

        def recv_step(i, c):
            k = shift_of(i)
            if layer == 0:
                meta_copy(k).wait_recv()
                table = table_ref[lax.rem(me + n - k, n)]
                sub = lax.broadcasted_iota(I32, (8, slot_cap), 0)
                parts = jnp.where(sub == 0, table & 255, jnp.where(sub == 1, table >> 8, 0))
                got = meta_in[k - 1]
                found = dot(parts.astype(F32).astype(BF16), one_hot(slot_cap, got[0:1]))
                row_ids[k - 1] = (found[0:1] + 256.0 * found[1:2]).astype(I32)
                flag_own[...] = jnp.maximum(flag_own[...], got[1:2, :LANES])
            data_copy(layer, k).wait_recv()
            add_rows(recv[layer, k - 1], row_ids[k - 1])
            return c

        lax.fori_loop(0, peers, recv_step, 0)

    spare = recv.shape[2] - cap
    recv[:, :, cap:, :] = jnp.zeros((2, peers, spare, hid), BF16)
    for c in range(chunks):
        part = slice(c * ROW_CHUNK, (c + 1) * ROW_CHUNK)
        mt[:, part] = dot_tn(msg1_ref[...], feat_ref[:, part]).astype(BF16)
    pl.semaphore_wait(barrier, n - 1 + groups - 1)

    def start_meta(i, c):
        meta_copy(shift_of(i)).start()
        return c

    lax.fori_loop(0, peers, start_meta, 0)
    layer_body(0)

    for c in range(chunks):
        part = slice(c * ROW_CHUNK, (c + 1) * ROW_CHUNK)
        hidden[part] = jnp.maximum(acc[part], 0.0).astype(BF16)
        mt[:, part] = lax.dot_general(msg2_ref[...], hidden[part], (((0,), (1,)), ((), ())), preferred_element_type=F32).astype(BF16)

    def start_flag(j, c):
        flag_copy(j).start()
        return c

    lax.fori_loop(1, groups, start_flag, 0)
    layer_body(1)

    out_ref[...] = acc[...].astype(BF16)

    def end_flag(j, seen):
        copy = flag_copy(j)
        copy.wait_recv()
        seen = jnp.maximum(seen, flag_in[j - 1])
        copy.wait_send()
        return seen

    flag_ref[0] = jnp.max(lax.fori_loop(1, groups, end_flag, flag_own[...]))

    def end_send(k, c):
        meta_copy(k).wait_send()
        data_copy(0, k).wait_send()
        data_copy(1, k).wait_send()
        return c

    lax.fori_loop(1, n, end_send, 0)


def solution(mesh):
    row_spec = P(("batch", "graph"), None)
    full_spec = P(None, None)
    table_spec = P(("batch", "graph"), None, None)
    n, groups = mesh.shape["graph"], mesh.shape["batch"]

    def plain_layer(h_loc, w_msg, w_self, src_idx, slot_idx, edge_w, recv_idx):
        rows_dev = h_loc.shape[0]
        messages = jnp.dot(h_loc, w_msg, preferred_element_type=F32).astype(BF16)
        weighted = messages[src_idx].astype(F32) * edge_w
        partial = jax.ops.segment_sum(weighted, slot_idx, num_segments=recv_idx.shape[0]).astype(BF16)
        received = lax.all_to_all(partial, "graph", 0, 0, tiled=True)
        agg_sum = jax.ops.segment_sum(received.astype(F32), recv_idx, num_segments=rows_dev + 1)
        self_term = jnp.dot(h_loc, w_self, preferred_element_type=F32)
        return jax.nn.relu(self_term + agg_sum[:rows_dev]).astype(BF16)

    def local_step(features, w_msg1, w_self1, w_msg2, w_self2, src_local, send_slot, edge_weight, recv_row):
        rows_dev, hid = features.shape[0], w_msg1.shape[1]
        slot_cap = recv_row.shape[2]
        edges = src_local.shape[1]
        peers = n - 1
        cap, lanes_cap = slot_cap * 23 // 32, slot_cap * 3 // 4
        width = PAIR_ROWS * LANES
        own_width = OWN_ROWS * LANES
        ranges = rows_dev // OWN_SPAN
        own_tiles = ranges * (edges * 3 // 5 // ranges // own_width)

        me = lax.axis_index("graph")
        slots, sources = send_slot.reshape(-1), src_local.reshape(-1)
        owner, offset = slots // slot_cap, slots % slot_cap
        rank = lax.rem(owner - me + 2 * n - 1, n)
        inner = jnp.where(rank == peers, sources * slot_cap + offset, offset * rows_dev + sources)
        key = rank * (slot_cap * rows_dev) + inner
        key, weight = lax.sort((key, edge_weight.reshape(-1)), num_keys=1, is_stable=False)

        vmem, smem = pl.BlockSpec(memory_space=pltpu.VMEM), pl.BlockSpec(memory_space=pltpu.SMEM)
        pair = lambda dtype: jax.ShapeDtypeStruct((peers, 1, width), dtype)
        own = lambda dtype: jax.ShapeDtypeStruct((own_tiles, 1, own_width), dtype)
        src, live, wgt, meta, own_src, own_slot, own_w, table = pl.pallas_call(
            functools.partial(prep_kernel, peers, slot_cap, rows_dev, cap),
            out_shape=(
                pair(I32), pair(I32), pair(F32), jax.ShapeDtypeStruct((peers, 8, lanes_cap), I32), own(I32), own(I32), own(F32),
                jax.ShapeDtypeStruct((n, 1, slot_cap), I32),
            ),
            in_specs=[vmem] * 4,
            out_specs=[vmem] * 8,
            scratch_shapes=[pltpu.VMEM((n, width), I32), pltpu.VMEM((n, width), F32), pltpu.VMEM((own_tiles, own_width), I32)],
            name="edge_windows",
        )(key.reshape(-1, LANES), key.reshape(-1, 1, LANES), weight.reshape(-1, 1, LANES), recv_row[0])

        out, flag = pl.pallas_call(
            functools.partial(gnn_kernel, n, groups, cap),
            out_shape=(jax.ShapeDtypeStruct((rows_dev, hid), BF16), jax.ShapeDtypeStruct((1,), I32)),
            in_specs=[vmem] * 13,
            out_specs=[vmem, smem],
            scratch_shapes=[
                pltpu.VMEM((hid, rows_dev), BF16),
                pltpu.VMEM((rows_dev, hid), BF16),
                pltpu.VMEM((rows_dev, hid), F32),
                pltpu.VMEM((hid, slot_cap), F32),
                pltpu.VMEM((2, peers, lanes_cap, hid), BF16),
                pltpu.VMEM((2, peers, lanes_cap, hid), BF16),
                pltpu.VMEM((peers, 8, lanes_cap), I32),
                pltpu.VMEM((peers, 1, lanes_cap), I32),
                pltpu.VMEM((8, LANES), I32),
                pltpu.VMEM((max(groups - 1, 1), 8, LANES), I32),
                pltpu.SemaphoreType.DMA((2, peers)),
                pltpu.SemaphoreType.DMA((2, peers)),
                pltpu.SemaphoreType.DMA((peers,)),
                pltpu.SemaphoreType.DMA((peers,)),
                pltpu.SemaphoreType.DMA((max(groups - 1, 1),)),
                pltpu.SemaphoreType.DMA((max(groups - 1, 1),)),
            ],
            compiler_params=pltpu.CompilerParams(collective_id=0, has_side_effects=True, vmem_limit_bytes=56 * 2**20),
            name="gnn_layers",
        )(features.T, w_msg1, w_self1, w_msg2, w_self2, src, live, wgt, own_src, own_slot, own_w, meta, table)

        def plain():
            args = src_local[0], send_slot[0], edge_weight[0][:, None], recv_row[0].reshape(-1)
            extra = features.shape[1] - hid
            grow = lambda w: jnp.pad(w, ((0, extra), (0, 0)))
            msg, own_part = jnp.stack([w_msg1, grow(w_msg2)]), jnp.stack([w_self1, grow(w_self2)])

            def step(h, weights):
                return jnp.pad(plain_layer(h, *weights, *args), ((0, 0), (0, extra))), None

            hidden, _ = lax.scan(step, features, (msg, own_part))
            return hidden[:, :hid]

        return jnp.maximum(lax.cond(flag[0] > 0, plain, lambda: out), 0)

    return jax.shard_map(local_step, mesh=mesh, in_specs=(row_spec, full_spec, full_spec, full_spec, full_spec, row_spec, row_spec, row_spec, table_spec), out_specs=row_spec, check_vma=False)
```
